8 devices in a mesh: fsdp: 8 (over z, y, x, core).
Axes of the slice: x: 2, y: 2, z: 1, core: 2. Of those that a mesh axis runs over, the one named last changes fastest.
Arguments:
- hidden: bfloat16 [24, 256, 2048], P('fsdp')
- grad_out: bfloat16 [24, 256, 2048], P('fsdp')
- positions: int32 [24, 256], P('fsdp')
- norm1_gain: bfloat16 [2048], P('fsdp')
- norm2_gain: bfloat16 [2048], P('fsdp')
- q_norm_gain: bfloat16 [128], replicated
- k_norm_gain: bfloat16 [128], replicated
- w_q: bfloat16 [2048, 2048], P('fsdp')
- w_k: bfloat16 [2048, 1024], P('fsdp')
- w_v: bfloat16 [2048, 1024], P('fsdp')
- w_o: bfloat16 [2048, 2048], P('fsdp')
- w_gate: bfloat16 [2048, 6144], P('fsdp')
- w_up: bfloat16 [2048, 6144], P('fsdp')
- w_down: bfloat16 [6144, 2048], P('fsdp')
Outputs:
- output 1: bfloat16 [24, 256, 2048], P('fsdp')
- output 2: bfloat16 [24, 256, 2048], P('fsdp')
- output 3: float32 [2048], P('fsdp')
- output 4: float32 [2048], P('fsdp')
- output 5: float32 [128], replicated
- output 6: float32 [128], replicated
- output 7: float32 [2048, 2048], P('fsdp')
- output 8: float32 [2048, 1024], P('fsdp')
- output 9: float32 [2048, 1024], P('fsdp')
- output 10: float32 [2048, 2048], P('fsdp')
- output 11: float32 [2048, 6144], P('fsdp')
- output 12: float32 [2048, 6144], P('fsdp')
- output 13: float32 [6144, 2048], P('fsdp')
All inputs are finite; a program needn't handle non-finite values.
Results may differ from the reference program's by a relative error of at most 0.02.
Values are sent between devices in bfloat16 or wider.
A program may use at most 1 GiB of HBM per device.

```python
import functools
import jax
import jax.numpy as jnp
from jax import lax

D = 2048
HEADS = 16
KV_HEADS = 8
HEAD = 128
FF = 6144
BATCH = 24
SEQ = 256
RMS_EPS = 1e-6
ROPE_THETA = 1000000.0
KV_GROUP = HEADS // KV_HEADS
TOKENS = BATCH * SEQ


def setup_inputs(seed: int = 0) -> dict:
    key_list = jax.random.split(jax.random.key(seed), 16)

    def normal_draw(key_index, arr_shape, std_scale):
        return (jax.random.normal(key_list[key_index], arr_shape, jnp.float32) * std_scale).astype(jnp.bfloat16)

    def gain_draw(key_index, arr_shape):
        return (1.0 + 0.3 * jax.random.normal(key_list[key_index], arr_shape, jnp.float32)).astype(jnp.bfloat16)

    start_key, stride_key = jax.random.split(key_list[2])
    start_pos = jax.random.randint(start_key, (BATCH, 1), 0, 4096)
    stride_pos = jax.random.randint(stride_key, (BATCH, SEQ), 1, 5)
    positions = (start_pos + jnp.cumsum(stride_pos, axis=1)).astype(jnp.int32)
    return {
        "hidden": normal_draw(0, (BATCH, SEQ, D), 1.0),
        "grad_out": normal_draw(1, (BATCH, SEQ, D), 1.0),
        "positions": positions,
        "norm1_gain": gain_draw(3, (D,)),
        "norm2_gain": gain_draw(4, (D,)),
        "q_norm_gain": gain_draw(5, (HEAD,)),
        "k_norm_gain": gain_draw(6, (HEAD,)),
        "w_q": normal_draw(7, (D, HEADS * HEAD), D ** -0.5),
        "w_k": normal_draw(8, (D, KV_HEADS * HEAD), D ** -0.5),
        "w_v": normal_draw(9, (D, KV_HEADS * HEAD), D ** -0.5),
        "w_o": normal_draw(10, (HEADS * HEAD, D), (HEADS * HEAD) ** -0.5),
        "w_gate": normal_draw(11, (D, FF), D ** -0.5),
        "w_up": normal_draw(12, (D, FF), D ** -0.5),
        "w_down": normal_draw(13, (FF, D), FF ** -0.5),
    }


def rms_scale(tensor):
    return lax.rsqrt(jnp.mean(tensor * tensor, axis=-1, keepdims=True) + RMS_EPS)


def rotate_half(tensor):
    half_dim = tensor.shape[-1] // 2
    return jnp.concatenate([-tensor[..., half_dim:], tensor[..., :half_dim]], axis=-1)


def attend_one(operands):
    q_seq, k_seq, v_seq = operands
    scores = jnp.einsum("skgd,tkd->kgst", q_seq.astype(jnp.float32), k_seq.astype(jnp.float32)) * (HEAD ** -0.5)
    causal = jnp.arange(SEQ)[:, None] >= jnp.arange(SEQ)[None, :]
    scores = jnp.where(causal, scores, -1e30)
    attn_probs = jax.nn.softmax(scores, axis=-1).astype(jnp.bfloat16)
    return jnp.einsum("kgst,tkd->skgd", attn_probs.astype(jnp.float32), v_seq.astype(jnp.float32)).astype(jnp.bfloat16)


def head_norm_rope(projected, num_heads, gain_vec, cos_t, sin_t):
    heads_float = projected.reshape(TOKENS, num_heads, HEAD).astype(jnp.float32)
    scaled = heads_float * rms_scale(heads_float) * gain_vec.astype(jnp.float32)
    return (scaled * cos_t + rotate_half(scaled) * sin_t).astype(jnp.bfloat16)


def layer_forward(positions, hidden, norm1_gain, norm2_gain, q_norm_gain, k_norm_gain, w_q, w_k, w_v, w_o, w_gate, w_up, w_down):
    x_float = hidden.reshape(TOKENS, D).astype(jnp.float32)
    normed = (x_float * rms_scale(x_float) * norm1_gain.astype(jnp.float32)).astype(jnp.bfloat16)
    q_proj = jnp.dot(normed, w_q, preferred_element_type=jnp.float32).astype(jnp.bfloat16)
    k_proj = jnp.dot(normed, w_k, preferred_element_type=jnp.float32).astype(jnp.bfloat16)
    v_proj = jnp.dot(normed, w_v, preferred_element_type=jnp.float32).astype(jnp.bfloat16)
    inv_freq = ROPE_THETA ** (-2.0 * jnp.arange(HEAD // 2, dtype=jnp.float32) / HEAD)
    rope_angle = positions.reshape(TOKENS, 1).astype(jnp.float32) * inv_freq
    cos_t = jnp.concatenate([jnp.cos(rope_angle), jnp.cos(rope_angle)], axis=-1)[:, None, :]
    sin_t = jnp.concatenate([jnp.sin(rope_angle), jnp.sin(rope_angle)], axis=-1)[:, None, :]
    q_rot = head_norm_rope(q_proj, HEADS, q_norm_gain, cos_t, sin_t)
    k_rot = head_norm_rope(k_proj, KV_HEADS, k_norm_gain, cos_t, sin_t)
    attn_ctx = lax.map(attend_one, (q_rot.reshape(BATCH, SEQ, KV_HEADS, KV_GROUP, HEAD), k_rot.reshape(BATCH, SEQ, KV_HEADS, HEAD), v_proj.reshape(BATCH, SEQ, KV_HEADS, HEAD)))
    attn_out = jnp.dot(attn_ctx.reshape(TOKENS, HEADS * HEAD), w_o, preferred_element_type=jnp.float32).astype(jnp.bfloat16)
    resid_float = (x_float + attn_out.astype(jnp.float32)).astype(jnp.bfloat16).astype(jnp.float32)
    mlp_in = (resid_float * rms_scale(resid_float) * norm2_gain.astype(jnp.float32)).astype(jnp.bfloat16)
    gate_proj = jnp.dot(mlp_in, w_gate, preferred_element_type=jnp.float32).astype(jnp.bfloat16)
    up_proj = jnp.dot(mlp_in, w_up, preferred_element_type=jnp.float32).astype(jnp.bfloat16)
    mlp_act = (jax.nn.silu(gate_proj.astype(jnp.float32)) * up_proj.astype(jnp.float32)).astype(jnp.bfloat16)
    down_proj = jnp.dot(mlp_act, w_down, preferred_element_type=jnp.float32).astype(jnp.bfloat16)
    layer_out = (resid_float + down_proj.astype(jnp.float32)).astype(jnp.bfloat16)
    return layer_out.reshape(BATCH, SEQ, D)


def mean_grad(grad_val):
    return grad_val.astype(jnp.float32) / TOKENS


def reference(hidden, grad_out, positions, norm1_gain, norm2_gain, q_norm_gain, k_norm_gain, w_q, w_k, w_v, w_o, w_gate, w_up, w_down):
    layer_out, pullback = jax.vjp(functools.partial(layer_forward, positions), hidden, norm1_gain, norm2_gain, q_norm_gain, k_norm_gain, w_q, w_k, w_v, w_o, w_gate, w_up, w_down)
    all_grads = pullback(grad_out)
    return (layer_out, all_grads[0].astype(jnp.bfloat16), mean_grad(all_grads[1]), mean_grad(all_grads[2]), mean_grad(all_grads[3]), mean_grad(all_grads[4]), mean_grad(all_grads[5]), mean_grad(all_grads[6]), mean_grad(all_grads[7]), mean_grad(all_grads[8]), mean_grad(all_grads[9]), mean_grad(all_grads[10]), mean_grad(all_grads[11]))
```

```python
import jax
import jax.numpy as jnp
from jax import lax
from jax.sharding import PartitionSpec as P


RMS_EPS = 1e-6
ROPE_THETA = 1000000.0


def rms_scale(tensor):
    return lax.rsqrt(jnp.mean(tensor * tensor, axis=-1, keepdims=True) + RMS_EPS)


def norm_backward(d_unit, unit_val, scale_val):
    return scale_val * (d_unit - unit_val * jnp.mean(d_unit * unit_val, axis=-1, keepdims=True))


def rotate_half(tensor):
    half_dim = tensor.shape[-1] // 2
    return jnp.concatenate([-tensor[..., half_dim:], tensor[..., :half_dim]], axis=-1)


def matmul(left_op, right_op):
    return jnp.dot(left_op, right_op, preferred_element_type=jnp.float32)


def matmul_tn(left_op, right_op):
    return lax.dot_general(left_op, right_op, (((0,), (0,)), ((), ())), preferred_element_type=jnp.float32)


def matmul_nt(left_op, right_op):
    return lax.dot_general(left_op, right_op, (((1,), (1,)), ((), ())), preferred_element_type=jnp.float32)


def rope_tables(positions, head_dim):
    inv_freq = ROPE_THETA ** (-2.0 * jnp.arange(head_dim // 2, dtype=jnp.float32) / head_dim)
    rope_angle = positions.reshape(-1, 1).astype(jnp.float32) * inv_freq
    cos_half = jnp.cos(rope_angle)
    sin_half = jnp.sin(rope_angle)
    cos_t = jnp.concatenate([cos_half, cos_half], axis=-1)[:, None, :]
    sin_t = jnp.concatenate([sin_half, sin_half], axis=-1)[:, None, :]
    return cos_t, sin_t


def head_norm_rope(projected, num_heads, head_dim, gain_vec, cos_t, sin_t):
    heads_float = projected.reshape(projected.shape[0], num_heads, head_dim).astype(jnp.float32)
    head_scale = rms_scale(heads_float)
    head_unit = heads_float * head_scale
    scaled = head_unit * gain_vec.astype(jnp.float32)
    rotated = (scaled * cos_t + rotate_half(scaled) * sin_t).astype(jnp.bfloat16)
    return rotated, head_unit, head_scale


def head_norm_rope_backward(d_rotated, head_unit, head_scale, gain_vec, cos_t, sin_t):
    d_scaled = d_rotated * cos_t - rotate_half(d_rotated * sin_t)
    d_gain = jnp.sum(d_scaled * head_unit, axis=(0, 1))
    d_projected = norm_backward(d_scaled * gain_vec.astype(jnp.float32), head_unit, head_scale)
    return d_projected.reshape(d_projected.shape[0], -1).astype(jnp.bfloat16), d_gain


NEG = -1e30


def attention_forward(x_float, positions, weights, batch_local, seq_len):
    norm1_gain, q_norm_gain, k_norm_gain, w_q, w_k, w_v = weights
    tokens = x_float.shape[0]
    head_dim = q_norm_gain.shape[0]
    num_heads = w_q.shape[1] // head_dim
    kv_heads = w_k.shape[1] // head_dim
    x_scale = rms_scale(x_float)
    x_unit = x_float * x_scale
    normed = (x_unit * norm1_gain.astype(jnp.float32)).astype(jnp.bfloat16)
    q_proj = matmul(normed, w_q).astype(jnp.bfloat16)
    k_proj = matmul(normed, w_k).astype(jnp.bfloat16)
    v_proj = matmul(normed, w_v).astype(jnp.bfloat16)
    cos_t, sin_t = rope_tables(positions, head_dim)
    q_rot, q_unit, q_scale = head_norm_rope(q_proj, num_heads, head_dim, q_norm_gain, cos_t, sin_t)
    k_rot, k_unit, k_scale = head_norm_rope(k_proj, kv_heads, head_dim, k_norm_gain, cos_t, sin_t)
    q_grouped = q_rot.reshape(batch_local, seq_len, kv_heads, num_heads // kv_heads, head_dim)
    k_seq = k_rot.reshape(batch_local, seq_len, kv_heads, head_dim)
    v_seq = v_proj.reshape(batch_local, seq_len, kv_heads, head_dim)
    scores = jnp.einsum("bskgd,btkd->bksgt", q_grouped, k_seq, preferred_element_type=jnp.float32) * (head_dim ** -0.5)
    causal = (jnp.arange(seq_len)[:, None] >= jnp.arange(seq_len)[None, :])[:, None, :]
    attn_probs = jax.nn.softmax(jnp.where(causal, scores, NEG), axis=-1)
    attn_ctx = jnp.einsum("bksgt,btkd->bskgd", attn_probs.astype(jnp.bfloat16), v_seq, preferred_element_type=jnp.float32).astype(jnp.bfloat16).reshape(tokens, num_heads * head_dim)
    saved = (x_unit, x_scale, normed, cos_t, sin_t, q_unit, q_scale, k_unit, k_scale, q_grouped, k_seq, v_seq, attn_probs)
    return attn_ctx, saved


def attention_backward(d_attn_ctx, saved, q_norm_gain, k_norm_gain):
    _, _, _, cos_t, sin_t, q_unit, q_scale, k_unit, k_scale, q_grouped, k_seq, v_seq, attn_probs = saved
    batch_local, seq_len, kv_heads, kv_group, head_dim = q_grouped.shape
    tokens = batch_local * seq_len
    num_heads = kv_heads * kv_group
    d_attn_ctx = d_attn_ctx.reshape(batch_local, seq_len, kv_heads, kv_group, head_dim)
    d_value = jnp.einsum("bksgt,bskgd->btkd", attn_probs.astype(jnp.bfloat16), d_attn_ctx, preferred_element_type=jnp.float32).astype(jnp.bfloat16).reshape(tokens, kv_heads * head_dim)
    d_probs = jnp.einsum("bskgd,btkd->bksgt", d_attn_ctx, v_seq, preferred_element_type=jnp.float32)
    d_scores = attn_probs * (d_probs - jnp.sum(attn_probs * d_probs, axis=-1, keepdims=True))
    d_scores = (d_scores * (head_dim ** -0.5)).astype(jnp.bfloat16)
    d_q_rot = jnp.einsum("bksgt,btkd->bskgd", d_scores, k_seq, preferred_element_type=jnp.float32).reshape(tokens, num_heads, head_dim)
    d_k_rot = jnp.einsum("bksgt,bskgd->btkd", d_scores, q_grouped, preferred_element_type=jnp.float32).reshape(tokens, kv_heads, head_dim)
    d_query, grad_qgain = head_norm_rope_backward(d_q_rot, q_unit, q_scale, q_norm_gain, cos_t, sin_t)
    d_key, grad_kgain = head_norm_rope_backward(d_k_rot, k_unit, k_scale, k_norm_gain, cos_t, sin_t)
    return d_query, d_key, d_value, grad_qgain, grad_kgain


def pick(bit, first, second):
    return jnp.where(bit == 0, first, second), jnp.where(bit == 0, second, first)


def solution(mesh):
    axis_name = mesh.axis_names[0]
    group_size = mesh.shape[axis_name]
    sharded = P(axis_name)
    in_specs = (sharded, sharded, sharded, sharded, sharded, P(), P()) + (sharded,) * 7
    out_specs = (sharded, sharded, sharded, sharded, P(), P()) + (sharded,) * 7
    CORE, XDIR, YDIR = 1, 2, 4

    def swap(value, mask):
        return lax.ppermute(value, axis_name, [(j, j ^ mask) for j in range(group_size)])

    def gather_rows(row_shard):
        return lax.all_gather(row_shard, axis_name, axis=0, tiled=True)

    def device_step(hidden, grad_out, positions, norm1_gain, norm2_gain, q_norm_gain, k_norm_gain, w_q, w_k, w_v, w_o, w_gate, w_up, w_down):
        batch_local, seq_len, width = hidden.shape
        tokens = batch_local * seq_len
        me = lax.axis_index(axis_name)
        c_bit, x_bit, y_bit = me % 2, (me // 2) % 2, me // 4
        ff_block = w_down.shape[0]
        rows = w_gate.shape[0]

        def row_tokens(own):
            pair = jnp.concatenate([own, swap(own, XDIR)], axis=0)
            return jnp.concatenate([pair, swap(pair, CORE)], axis=0)

        def quarter_columns(shard):
            blk = [shard[:, j * ff_block:(j + 1) * ff_block] for j in range(8)]
            first = jnp.concatenate([blk[0], blk[1], blk[4], blk[5]], axis=1)
            second = jnp.concatenate([blk[2], blk[3], blk[6], blk[7]], axis=1)
            keep, send = pick(x_bit, first, second)
            got = swap(send, XDIR)
            row0, row1 = pick(x_bit, keep, got)
            both = jnp.concatenate([row0, row1], axis=0)
            col = [both[:, j * ff_block:(j + 1) * ff_block] for j in range(4)]
            keep, send = pick(c_bit, jnp.concatenate([col[0], col[2]], axis=1), jnp.concatenate([col[1], col[3]], axis=1))
            got = swap(send, CORE)
            core0, core1 = pick(c_bit, keep, got)
            four = jnp.concatenate([core0[:rows], core1[:rows], core0[rows:], core1[rows:]], axis=0)
            got = swap(four, YDIR)
            return jnp.concatenate(pick(y_bit, four, got), axis=0)

        def row_sum(partial_rows):
            far = partial_rows(2 * tokens, 4 * tokens)
            from_core = swap(far, CORE)
            side = partial_rows(tokens, 2 * tokens) + from_core[tokens:]
            from_x = swap(side, XDIR)
            total = partial_rows(0, tokens) + from_core[:tokens]
            return total, from_x

        def scatter_columns(left_send, left_keep, right):
            part = matmul_tn(left_send, right)
            got = swap(part, YDIR)
            mine = matmul_tn(left_keep, right) + got
            blk = [mine[j * rows:(j + 1) * rows] for j in range(4)]
            keep, send = pick(c_bit, jnp.concatenate([blk[0], blk[2]], axis=0), jnp.concatenate([blk[1], blk[3]], axis=0))
            got = swap(send, CORE)
            core0, core1 = pick(c_bit, keep, got)
            both = jnp.concatenate([core0, core1], axis=1)
            keep, send = pick(x_bit, both[:rows], both[rows:])
            got = swap(send, XDIR)
            x0, x1 = pick(x_bit, keep, got)
            parts = [x0[:, :ff_block], x0[:, 2 * ff_block:3 * ff_block], x1[:, :ff_block], x1[:, 2 * ff_block:3 * ff_block]]
            parts += [x0[:, ff_block:2 * ff_block], x0[:, 3 * ff_block:], x1[:, ff_block:2 * ff_block], x1[:, 3 * ff_block:]]
            return jnp.concatenate(parts, axis=1)

        gains = lax.all_gather(jnp.stack([norm1_gain, norm2_gain]), axis_name, axis=1, tiled=True)
        gain1, gain2 = gains[0].astype(jnp.float32), gains[1].astype(jnp.float32)
        full_q, full_k, full_v, full_o = gather_rows(w_q), gather_rows(w_k), gather_rows(w_v), gather_rows(w_o)
        gate_q = quarter_columns(w_gate)
        up_q = quarter_columns(w_up)
        down_q = jnp.concatenate(pick(y_bit, w_down, swap(w_down, YDIR)), axis=0)
        dy_flat = grad_out.reshape(tokens, width)
        dy_row = row_tokens(dy_flat)

        x_float = hidden.reshape(tokens, width).astype(jnp.float32)
        attn_ctx, saved = attention_forward(x_float, positions, (gains[0], q_norm_gain, k_norm_gain, full_q, full_k, full_v), batch_local, seq_len)
        attn_out = matmul(attn_ctx, full_o).astype(jnp.bfloat16)
        resid_float = (x_float + attn_out.astype(jnp.float32)).astype(jnp.bfloat16).astype(jnp.float32)
        r_scale = rms_scale(resid_float)
        r_unit = resid_float * r_scale
        mlp_in = row_tokens((r_unit * gain2).astype(jnp.bfloat16))

        gate_proj = matmul(mlp_in, gate_q).astype(jnp.bfloat16)
        up_proj = matmul(mlp_in, up_q).astype(jnp.bfloat16)
        gate_float = gate_proj.astype(jnp.float32)
        up_float = up_proj.astype(jnp.float32)
        mlp_act = (jax.nn.silu(gate_float) * up_float).astype(jnp.bfloat16)

        d_mlp_act = matmul_nt(dy_row, down_q)
        gate_sig = jax.nn.sigmoid(gate_float)
        d_up = (d_mlp_act * gate_float * gate_sig).astype(jnp.bfloat16)
        d_gate = (d_mlp_act * up_float * gate_sig * (1.0 + gate_float * (1.0 - gate_sig))).astype(jnp.bfloat16)
        inv_tokens = 1.0 / (tokens * group_size)
        act_keep, act_send = pick(y_bit, mlp_act[:, :ff_block], mlp_act[:, ff_block:])
        down_part = matmul_tn(act_send, dy_row)
        down_got = swap(down_part, YDIR)
        grad_down = (matmul_tn(act_keep, dy_row) + down_got) * inv_tokens

        d_mlp_in, dm_from_x = row_sum(lambda lo, hi: matmul_nt(d_gate[lo:hi], gate_q) + matmul_nt(d_up[lo:hi], up_q))
        d_mlp_in = d_mlp_in + dm_from_x
        in_keep, in_send = pick(y_bit, mlp_in[:, :width // 2], mlp_in[:, width // 2:])
        grad_gate = scatter_columns(in_send, in_keep, d_gate) * inv_tokens
        grad_up = scatter_columns(in_send, in_keep, d_up) * inv_tokens

        down_total, down_from_x = row_sum(lambda lo, hi: matmul(mlp_act[lo:hi], down_q))

        grad_norm2 = jnp.sum(d_mlp_in * r_unit, axis=0)
        d_resid = dy_flat.astype(jnp.float32) + norm_backward(d_mlp_in * gain2, r_unit, r_scale)
        d_resid_bf = d_resid.astype(jnp.bfloat16)
        d_attn_ctx = matmul_nt(d_resid_bf, full_o).astype(jnp.bfloat16)
        down_from_x, d_attn_ctx = lax.optimization_barrier((down_from_x, d_attn_ctx))
        down_proj = (down_total + down_from_x).astype(jnp.bfloat16)
        layer_out = (resid_float + down_proj.astype(jnp.float32)).astype(jnp.bfloat16).reshape(hidden.shape)
        grad_wo = lax.psum_scatter(matmul_tn(attn_ctx, d_resid_bf) * inv_tokens, axis_name, scatter_dimension=0, tiled=True)
        d_query, d_key, d_value, grad_qgain, grad_kgain = attention_backward(d_attn_ctx, saved, q_norm_gain, k_norm_gain)
        x_unit, x_scale, normed = saved[:3]
        grad_wv = lax.psum_scatter(matmul_tn(normed, d_value) * inv_tokens, axis_name, scatter_dimension=0, tiled=True)
        grad_wk = lax.psum_scatter(matmul_tn(normed, d_key) * inv_tokens, axis_name, scatter_dimension=0, tiled=True)
        grad_wq = lax.psum_scatter(matmul_tn(normed, d_query) * inv_tokens, axis_name, scatter_dimension=0, tiled=True)
        d_normed = matmul_nt(d_query, full_q) + matmul_nt(d_key, full_k) + matmul_nt(d_value, full_v)
        grad_norm1 = jnp.sum(d_normed * x_unit, axis=0)
        d_hidden = (d_resid + norm_backward(d_normed * gain1, x_unit, x_scale)).astype(jnp.bfloat16).reshape(hidden.shape)

        small = lax.psum(jnp.concatenate([grad_norm1, grad_norm2, grad_qgain, grad_kgain]) * inv_tokens, axis_name)
        head_dim = q_norm_gain.shape[0]
        own1 = lax.dynamic_slice_in_dim(small, me * rows, rows)
        own2 = lax.dynamic_slice_in_dim(small, width + me * rows, rows)
        gq = small[2 * width:2 * width + head_dim]
        gk = small[2 * width + head_dim:]
        return (layer_out, d_hidden, own1, own2, gq, gk, grad_wq, grad_wk, grad_wv, grad_wo, grad_gate, grad_up, grad_down)

    return jax.shard_map(device_step, mesh=mesh, in_specs=in_specs, out_specs=out_specs, check_vma=False)
```

```python
import jax
import jax.numpy as jnp
from jax import lax
from jax.sharding import PartitionSpec as P


RMS_EPS = 1e-6
ROPE_THETA = 1000000.0


def rms_scale(tensor):
    return lax.rsqrt(jnp.mean(tensor * tensor, axis=-1, keepdims=True) + RMS_EPS)


def norm_backward(d_unit, unit_val, scale_val):
    return scale_val * (d_unit - unit_val * jnp.mean(d_unit * unit_val, axis=-1, keepdims=True))


def rotate_half(tensor):
    half_dim = tensor.shape[-1] // 2
    return jnp.concatenate([-tensor[..., half_dim:], tensor[..., :half_dim]], axis=-1)


def matmul(left_op, right_op):
    return jnp.dot(left_op, right_op, preferred_element_type=jnp.float32)


def matmul_tn(left_op, right_op):
    return lax.dot_general(left_op, right_op, (((0,), (0,)), ((), ())), preferred_element_type=jnp.float32)


def matmul_nt(left_op, right_op):
    return lax.dot_general(left_op, right_op, (((1,), (1,)), ((), ())), preferred_element_type=jnp.float32)


def rope_tables(positions, head_dim):
    inv_freq = ROPE_THETA ** (-2.0 * jnp.arange(head_dim // 2, dtype=jnp.float32) / head_dim)
    rope_angle = positions.reshape(-1, 1).astype(jnp.float32) * inv_freq
    cos_half = jnp.cos(rope_angle)
    sin_half = jnp.sin(rope_angle)
    cos_t = jnp.concatenate([cos_half, cos_half], axis=-1)[:, None, :]
    sin_t = jnp.concatenate([sin_half, sin_half], axis=-1)[:, None, :]
    return cos_t, sin_t


def head_norm_rope(projected, num_heads, head_dim, gain_vec, cos_t, sin_t):
    heads_float = projected.reshape(projected.shape[0], num_heads, head_dim).astype(jnp.float32)
    head_scale = rms_scale(heads_float)
    head_unit = heads_float * head_scale
    scaled = head_unit * gain_vec.astype(jnp.float32)
    rotated = (scaled * cos_t + rotate_half(scaled) * sin_t).astype(jnp.bfloat16)
    return rotated, head_unit, head_scale


def head_norm_rope_backward(d_rotated, head_unit, head_scale, gain_vec, cos_t, sin_t):
    d_scaled = d_rotated * cos_t - rotate_half(d_rotated * sin_t)
    d_gain = jnp.sum(d_scaled * head_unit, axis=(0, 1))
    d_projected = norm_backward(d_scaled * gain_vec.astype(jnp.float32), head_unit, head_scale)
    return d_projected.reshape(d_projected.shape[0], -1).astype(jnp.bfloat16), d_gain


NEG = -1e30


def attention_forward(x_float, positions, weights, batch_local, seq_len):
    norm1_gain, q_norm_gain, k_norm_gain, w_q, w_k, w_v = weights
    tokens = x_float.shape[0]
    head_dim = q_norm_gain.shape[0]
    num_heads = w_q.shape[1] // head_dim
    kv_heads = w_k.shape[1] // head_dim
    x_scale = rms_scale(x_float)
    x_unit = x_float * x_scale
    normed = (x_unit * norm1_gain.astype(jnp.float32)).astype(jnp.bfloat16)
    q_proj = matmul(normed, w_q).astype(jnp.bfloat16)
    k_proj = matmul(normed, w_k).astype(jnp.bfloat16)
    v_proj = matmul(normed, w_v).astype(jnp.bfloat16)
    cos_t, sin_t = rope_tables(positions, head_dim)
    q_rot, q_unit, q_scale = head_norm_rope(q_proj, num_heads, head_dim, q_norm_gain, cos_t, sin_t)
    k_rot, k_unit, k_scale = head_norm_rope(k_proj, kv_heads, head_dim, k_norm_gain, cos_t, sin_t)
    q_grouped = q_rot.reshape(batch_local, seq_len, kv_heads, num_heads // kv_heads, head_dim)
    k_seq = k_rot.reshape(batch_local, seq_len, kv_heads, head_dim)
    v_seq = v_proj.reshape(batch_local, seq_len, kv_heads, head_dim)
    scores = jnp.einsum("bskgd,btkd->bksgt", q_grouped, k_seq, preferred_element_type=jnp.float32) * (head_dim ** -0.5)
    causal = (jnp.arange(seq_len)[:, None] >= jnp.arange(seq_len)[None, :])[:, None, :]
    attn_probs = jax.nn.softmax(jnp.where(causal, scores, NEG), axis=-1)
    attn_ctx = jnp.einsum("bksgt,btkd->bskgd", attn_probs.astype(jnp.bfloat16), v_seq, preferred_element_type=jnp.float32).astype(jnp.bfloat16).reshape(tokens, num_heads * head_dim)
    saved = (x_unit, x_scale, normed, cos_t, sin_t, q_unit, q_scale, k_unit, k_scale, q_grouped, k_seq, v_seq, attn_probs)
    return attn_ctx, saved


def attention_backward(d_attn_ctx, saved, q_norm_gain, k_norm_gain):
    _, _, _, cos_t, sin_t, q_unit, q_scale, k_unit, k_scale, q_grouped, k_seq, v_seq, attn_probs = saved
    batch_local, seq_len, kv_heads, kv_group, head_dim = q_grouped.shape
    tokens = batch_local * seq_len
    num_heads = kv_heads * kv_group
    d_attn_ctx = d_attn_ctx.reshape(batch_local, seq_len, kv_heads, kv_group, head_dim)
    d_value = jnp.einsum("bksgt,bskgd->btkd", attn_probs.astype(jnp.bfloat16), d_attn_ctx, preferred_element_type=jnp.float32).astype(jnp.bfloat16).reshape(tokens, kv_heads * head_dim)
    d_probs = jnp.einsum("bskgd,btkd->bksgt", d_attn_ctx, v_seq, preferred_element_type=jnp.float32)
    d_scores = attn_probs * (d_probs - jnp.sum(attn_probs * d_probs, axis=-1, keepdims=True))
    d_scores = (d_scores * (head_dim ** -0.5)).astype(jnp.bfloat16)
    d_q_rot = jnp.einsum("bksgt,btkd->bskgd", d_scores, k_seq, preferred_element_type=jnp.float32).reshape(tokens, num_heads, head_dim)
    d_k_rot = jnp.einsum("bksgt,bskgd->btkd", d_scores, q_grouped, preferred_element_type=jnp.float32).reshape(tokens, kv_heads, head_dim)
    d_query, grad_qgain = head_norm_rope_backward(d_q_rot, q_unit, q_scale, q_norm_gain, cos_t, sin_t)
    d_key, grad_kgain = head_norm_rope_backward(d_k_rot, k_unit, k_scale, k_norm_gain, cos_t, sin_t)
    return d_query, d_key, d_value, grad_qgain, grad_kgain


def pick(bit, first, second):
    return jnp.where(bit == 0, first, second), jnp.where(bit == 0, second, first)


def solution(mesh):
    axis_name = mesh.axis_names[0]
    group_size = mesh.shape[axis_name]
    sharded = P(axis_name)
    in_specs = (sharded, sharded, sharded, sharded, sharded, P(), P()) + (sharded,) * 7
    out_specs = (sharded, sharded, sharded, sharded, P(), P()) + (sharded,) * 7
    CORE, XDIR, YDIR = 1, 2, 4

    def swap(value, mask):
        return lax.ppermute(value, axis_name, [(j, j ^ mask) for j in range(group_size)])

    def gather_rows(row_shard):
        return lax.all_gather(row_shard, axis_name, axis=0, tiled=True)

    def device_step(hidden, grad_out, positions, norm1_gain, norm2_gain, q_norm_gain, k_norm_gain, w_q, w_k, w_v, w_o, w_gate, w_up, w_down):
        batch_local, seq_len, width = hidden.shape
        tokens = batch_local * seq_len
        me = lax.axis_index(axis_name)
        c_bit, x_bit, y_bit = me % 2, (me // 2) % 2, me // 4
        ff_block = w_down.shape[0]
        rows = w_gate.shape[0]

        def row_tokens(own):
            pair = jnp.concatenate([own, swap(own, XDIR)], axis=0)
            return jnp.concatenate([pair, swap(pair, CORE)], axis=0)

        def quarter_columns(shard):
            blk = [shard[:, j * ff_block:(j + 1) * ff_block] for j in range(8)]
            first = jnp.concatenate([blk[0], blk[1], blk[4], blk[5]], axis=1)
            second = jnp.concatenate([blk[2], blk[3], blk[6], blk[7]], axis=1)
            keep, send = pick(x_bit, first, second)
            got = swap(send, XDIR)
            row0, row1 = pick(x_bit, keep, got)
            both = jnp.concatenate([row0, row1], axis=0)
            col = [both[:, j * ff_block:(j + 1) * ff_block] for j in range(4)]
            keep, send = pick(c_bit, jnp.concatenate([col[0], col[2]], axis=1), jnp.concatenate([col[1], col[3]], axis=1))
            got = swap(send, CORE)
            core0, core1 = pick(c_bit, keep, got)
            four = jnp.concatenate([core0[:rows], core1[:rows], core0[rows:], core1[rows:]], axis=0)
            got = swap(four, YDIR)
            return jnp.concatenate(pick(y_bit, four, got), axis=0)

        def row_sum(partial_rows):
            far = partial_rows(2 * tokens, 4 * tokens)
            from_core = swap(far, CORE)
            side = partial_rows(tokens, 2 * tokens) + from_core[tokens:]
            from_x = swap(side, XDIR)
            total = partial_rows(0, tokens) + from_core[:tokens]
            return total, from_x

        def scatter_columns(left_send, left_keep, right):
            part = matmul_tn(left_send, right)
            got = swap(part, YDIR)
            mine = matmul_tn(left_keep, right) + got
            blk = [mine[j * rows:(j + 1) * rows] for j in range(4)]
            keep, send = pick(c_bit, jnp.concatenate([blk[0], blk[2]], axis=0), jnp.concatenate([blk[1], blk[3]], axis=0))
            got = swap(send, CORE)
            core0, core1 = pick(c_bit, keep, got)
            both = jnp.concatenate([core0, core1], axis=1)
            keep, send = pick(x_bit, both[:rows], both[rows:])
            got = swap(send, XDIR)
            x0, x1 = pick(x_bit, keep, got)
            parts = [x0[:, :ff_block], x0[:, 2 * ff_block:3 * ff_block], x1[:, :ff_block], x1[:, 2 * ff_block:3 * ff_block]]
            parts += [x0[:, ff_block:2 * ff_block], x0[:, 3 * ff_block:], x1[:, ff_block:2 * ff_block], x1[:, 3 * ff_block:]]
            return jnp.concatenate(parts, axis=1)

        gains = lax.all_gather(jnp.stack([norm1_gain, norm2_gain]), axis_name, axis=1, tiled=True)
        full_q, full_k, full_v, full_o = gather_rows(w_q), gather_rows(w_k), gather_rows(w_v), gather_rows(w_o)
        gate_own, down_own, gains = lax.optimization_barrier((w_gate, w_down, gains))
        gain1, gain2 = gains[0].astype(jnp.float32), gains[1].astype(jnp.float32)
        up_own, full_k = lax.optimization_barrier((w_up, full_k))
        dy_flat = grad_out.reshape(tokens, width)
        dy_own, full_q = lax.optimization_barrier((dy_flat, full_q))
        gate_q = quarter_columns(gate_own)
        up_q = quarter_columns(up_own)
        down_q = jnp.concatenate(pick(y_bit, down_own, swap(down_own, YDIR)), axis=0)
        dy_row = row_tokens(dy_own)

        x_float = hidden.reshape(tokens, width).astype(jnp.float32)
        attn_ctx, saved = attention_forward(x_float, positions, (gains[0], q_norm_gain, k_norm_gain, full_q, full_k, full_v), batch_local, seq_len)
        attn_out = matmul(attn_ctx, full_o).astype(jnp.bfloat16)
        resid_float = (x_float + attn_out.astype(jnp.float32)).astype(jnp.bfloat16).astype(jnp.float32)
        r_scale = rms_scale(resid_float)
        r_unit = resid_float * r_scale
        mlp_in = row_tokens((r_unit * gain2).astype(jnp.bfloat16))

        gate_proj = matmul(mlp_in, gate_q).astype(jnp.bfloat16)
        up_proj = matmul(mlp_in, up_q).astype(jnp.bfloat16)
        gate_float = gate_proj.astype(jnp.float32)
        up_float = up_proj.astype(jnp.float32)
        mlp_act = (jax.nn.silu(gate_float) * up_float).astype(jnp.bfloat16)

        d_mlp_act = matmul_nt(dy_row, down_q)
        gate_sig = jax.nn.sigmoid(gate_float)
        d_up = (d_mlp_act * gate_float * gate_sig).astype(jnp.bfloat16)
        d_gate = (d_mlp_act * up_float * gate_sig * (1.0 + gate_float * (1.0 - gate_sig))).astype(jnp.bfloat16)
        inv_tokens = 1.0 / (tokens * group_size)
        act_keep, act_send = pick(y_bit, mlp_act[:, :ff_block], mlp_act[:, ff_block:])
        down_part = matmul_tn(act_send, dy_row)
        down_got = swap(down_part, YDIR)
        grad_down = (matmul_tn(act_keep, dy_row) + down_got) * inv_tokens

        d_mlp_in, dm_from_x = row_sum(lambda lo, hi: matmul_nt(d_gate[lo:hi], gate_q) + matmul_nt(d_up[lo:hi], up_q))
        d_mlp_in = d_mlp_in + dm_from_x
        in_keep, in_send = pick(y_bit, mlp_in[:, :width // 2], mlp_in[:, width // 2:])
        grad_gate = scatter_columns(in_send, in_keep, d_gate) * inv_tokens
        grad_up = scatter_columns(in_send, in_keep, d_up) * inv_tokens

        down_total, down_from_x = row_sum(lambda lo, hi: matmul(mlp_act[lo:hi], down_q))

        grad_norm2 = jnp.sum(d_mlp_in * r_unit, axis=0)
        d_resid = dy_flat.astype(jnp.float32) + norm_backward(d_mlp_in * gain2, r_unit, r_scale)
        d_resid_bf = d_resid.astype(jnp.bfloat16)
        d_attn_ctx = matmul_nt(d_resid_bf, full_o).astype(jnp.bfloat16)
        down_from_x, _ = lax.optimization_barrier((down_from_x, d_attn_ctx))
        down_proj = (down_total + down_from_x).astype(jnp.bfloat16)
        layer_out = (resid_float + down_proj.astype(jnp.float32)).astype(jnp.bfloat16).reshape(hidden.shape)
        wo_part = matmul_tn(attn_ctx, d_resid_bf) * inv_tokens
        wo_part, d_attn_ctx = lax.optimization_barrier((wo_part, d_attn_ctx))
        grad_wo = lax.psum_scatter(wo_part, axis_name, scatter_dimension=0, tiled=True)
        d_query, d_key, d_value, grad_qgain, grad_kgain = attention_backward(d_attn_ctx, saved, q_norm_gain, k_norm_gain)
        x_unit, x_scale, normed = saved[:3]
        wv_part = matmul_tn(normed, d_value) * inv_tokens
        grad_wv = lax.psum_scatter(wv_part, axis_name, scatter_dimension=0, tiled=True)
        wk_part = matmul_tn(normed, d_key) * inv_tokens
        grad_wk = lax.psum_scatter(wk_part, axis_name, scatter_dimension=0, tiled=True)
        wq_part = matmul_tn(normed, d_query) * inv_tokens
        grad_wq = lax.psum_scatter(wq_part, axis_name, scatter_dimension=0, tiled=True)
        d_normed = matmul_nt(d_query, full_q) + matmul_nt(d_key, full_k) + matmul_nt(d_value, full_v)
        grad_norm1 = jnp.sum(d_normed * x_unit, axis=0)
        d_hidden = (d_resid + norm_backward(d_normed * gain1, x_unit, x_scale)).astype(jnp.bfloat16).reshape(hidden.shape)

        small = jnp.concatenate([grad_norm1, grad_norm2, grad_qgain, grad_kgain]) * inv_tokens
        for mask in (CORE, XDIR, YDIR):
            small = small + swap(small, mask)
        head_dim = q_norm_gain.shape[0]
        own1 = lax.dynamic_slice_in_dim(small, me * rows, rows)
        own2 = lax.dynamic_slice_in_dim(small, width + me * rows, rows)
        gq = small[2 * width:2 * width + head_dim]
        gk = small[2 * width + head_dim:]
        return (layer_out, d_hidden, own1, own2, gq, gk, grad_wq, grad_wk, grad_wv, grad_wo, grad_gate, grad_up, grad_down)

    return jax.shard_map(device_step, mesh=mesh, in_specs=in_specs, out_specs=out_specs, check_vma=False)
```

```python
import jax
import jax.numpy as jnp
from jax import lax
from jax.experimental import pallas as pl
from jax.experimental.pallas import tpu as pltpu
from jax.sharding import PartitionSpec as P


RMS_EPS = 1e-6
ROPE_THETA = 1000000.0
NEG = -1e30


def rms_scale(tensor):
    return lax.rsqrt(jnp.mean(tensor * tensor, axis=-1, keepdims=True) + RMS_EPS)


def norm_backward(d_unit, unit_val, scale_val):
    return scale_val * (d_unit - unit_val * jnp.mean(d_unit * unit_val, axis=-1, keepdims=True))


def matmul(left_op, right_op):
    return jnp.dot(left_op, right_op, preferred_element_type=jnp.float32)


def matmul_tn(left_op, right_op):
    return lax.dot_general(left_op, right_op, (((0,), (0,)), ((), ())), preferred_element_type=jnp.float32)


def matmul_nt(left_op, right_op):
    return lax.dot_general(left_op, right_op, (((1,), (1,)), ((), ())), preferred_element_type=jnp.float32)


def rope_tables(positions, head_dim):
    inv_freq = ROPE_THETA ** (-2.0 * jnp.arange(head_dim // 2, dtype=jnp.float32) / head_dim)
    rope_angle = positions.reshape(-1, 1).astype(jnp.float32) * inv_freq
    cos_half = jnp.cos(rope_angle)
    sin_half = jnp.sin(rope_angle)
    return jnp.concatenate([cos_half, cos_half], axis=-1), jnp.concatenate([-sin_half, sin_half], axis=-1)


def half_turn(tensor):
    return pltpu.roll(tensor, tensor.shape[-1] // 2, 1)


def head_unit(projected):
    heads = projected.astype(jnp.float32)
    scale = rms_scale(heads)
    return heads * scale, scale


def head_rope(unit, gain, cos_t, sin_t):
    scaled = unit * gain
    return (scaled * cos_t + half_turn(scaled) * sin_t).astype(jnp.bfloat16)


def head_backward(d_rot, unit, scale, gain, cos_t, sin_t):
    d_scaled = d_rot * cos_t + half_turn(d_rot * sin_t)
    d_gain = jnp.sum((d_scaled * unit).reshape(-1, 8, d_rot.shape[-1]), axis=0)
    return norm_backward(d_scaled * gain, unit, scale).astype(jnp.bfloat16), d_gain


def head_probs(q_rot, k_rot):
    seq_len, head_dim = q_rot.shape
    scores = matmul_nt(q_rot, k_rot) * (head_dim ** -0.5)
    query = lax.broadcasted_iota(jnp.int32, (seq_len, seq_len), 0)
    key = lax.broadcasted_iota(jnp.int32, (seq_len, seq_len), 1)
    scores = jnp.where(query >= key, scores, NEG)
    weight = jnp.exp(scores - jnp.max(scores, axis=-1, keepdims=True))
    return weight / jnp.sum(weight, axis=-1, keepdims=True)


def attention_forward_kernel(q_ref, k_ref, v_ref, cos_ref, sin_ref, qg_ref, kg_ref, ctx_ref):
    head_dim = k_ref.shape[1]
    cos_t, sin_t = cos_ref[...], sin_ref[...]
    q_gain, k_gain = qg_ref[...].astype(jnp.float32), kg_ref[...].astype(jnp.float32)
    k_rot = head_rope(head_unit(k_ref[...])[0], k_gain, cos_t, sin_t)
    for g in range(q_ref.shape[1] // head_dim):
        cols = slice(g * head_dim, (g + 1) * head_dim)
        q_rot = head_rope(head_unit(q_ref[:, cols])[0], q_gain, cos_t, sin_t)
        probs = head_probs(q_rot, k_rot).astype(jnp.bfloat16)
        ctx_ref[:, cols] = matmul(probs, v_ref[...]).astype(jnp.bfloat16)


def attention_backward_kernel(d_ref, q_ref, k_ref, v_ref, cos_ref, sin_ref, qg_ref, kg_ref, dq_ref, dk_ref, dv_ref, dqg_ref, dkg_ref):
    head_dim = k_ref.shape[1]
    cos_t, sin_t = cos_ref[...], sin_ref[...]
    q_gain, k_gain = qg_ref[...].astype(jnp.float32), kg_ref[...].astype(jnp.float32)
    k_unit, k_scale = head_unit(k_ref[...])
    k_rot = head_rope(k_unit, k_gain, cos_t, sin_t)
    d_k_rot = d_value = d_q_gain = 0.0
    for g in range(q_ref.shape[1] // head_dim):
        cols = slice(g * head_dim, (g + 1) * head_dim)
        q_unit, q_scale = head_unit(q_ref[:, cols])
        q_rot = head_rope(q_unit, q_gain, cos_t, sin_t)
        probs = head_probs(q_rot, k_rot)
        d_ctx = d_ref[:, cols]
        d_value = d_value + matmul_tn(probs.astype(jnp.bfloat16), d_ctx)
        d_probs = matmul_nt(d_ctx, v_ref[...])
        d_scores = probs * (d_probs - jnp.sum(probs * d_probs, axis=-1, keepdims=True))
        d_scores = (d_scores * (head_dim ** -0.5)).astype(jnp.bfloat16)
        d_k_rot = d_k_rot + matmul_tn(d_scores, q_rot)
        dq_ref[:, cols], part = head_backward(matmul(d_scores, k_rot), q_unit, q_scale, q_gain, cos_t, sin_t)
        d_q_gain = d_q_gain + part
    dqg_ref[...] = d_q_gain
    dk_ref[...], dkg_ref[...] = head_backward(d_k_rot, k_unit, k_scale, k_gain, cos_t, sin_t)
    dv_ref[...] = d_value.astype(jnp.bfloat16)


def attention_specs(q_proj, k_proj, seq_len, head_dim):
    tokens = q_proj.shape[0]
    kv_heads = k_proj.shape[1] // head_dim
    q_spec = pl.BlockSpec((seq_len, q_proj.shape[1] // kv_heads), lambda b, h: (b, h))
    k_spec = pl.BlockSpec((seq_len, head_dim), lambda b, h: (b, h))
    t_spec = pl.BlockSpec((seq_len, head_dim), lambda b, h: (b, 0))
    g_spec = pl.BlockSpec((1, head_dim), lambda b, h: (0, 0))
    return (tokens // seq_len, kv_heads), q_spec, k_spec, [q_spec, k_spec, k_spec, t_spec, t_spec, g_spec, g_spec]


def attention_forward(operands, seq_len):
    q_proj, k_proj, head_dim = operands[0], operands[1], operands[3].shape[1]
    grid, q_spec, _, in_specs = attention_specs(q_proj, k_proj, seq_len, head_dim)
    return pl.pallas_call(
        attention_forward_kernel, grid=grid, in_specs=in_specs, out_specs=q_spec,
        out_shape=jax.ShapeDtypeStruct(q_proj.shape, jnp.bfloat16),
        cost_estimate=pl.CostEstimate(flops=4 * q_proj.size * seq_len, bytes_accessed=8 * q_proj.size, transcendentals=0),
        name="attn_fwd",
    )(*operands)


def attention_backward(d_ctx, operands, seq_len):
    q_proj, k_proj, head_dim = operands[0], operands[1], operands[3].shape[1]
    grid, q_spec, k_spec, in_specs = attention_specs(q_proj, k_proj, seq_len, head_dim)
    gain_spec = pl.BlockSpec((8, head_dim), lambda b, h: (b * grid[1] + h, 0))
    gain_shape = jax.ShapeDtypeStruct((8 * grid[0] * grid[1], head_dim), jnp.float32)
    dq, dk, dv, dqg, dkg = pl.pallas_call(
        attention_backward_kernel, grid=grid, in_specs=[q_spec] + in_specs,
        out_specs=[q_spec, k_spec, k_spec, gain_spec, gain_spec],
        out_shape=[jax.ShapeDtypeStruct(q_proj.shape, jnp.bfloat16)] + [jax.ShapeDtypeStruct(k_proj.shape, jnp.bfloat16)] * 2 + [gain_shape] * 2,
        cost_estimate=pl.CostEstimate(flops=10 * q_proj.size * seq_len, bytes_accessed=12 * q_proj.size, transcendentals=0),
        name="attn_bwd",
    )(d_ctx, *operands)
    return dq, dk, dv, jnp.sum(dqg, axis=0), jnp.sum(dkg, axis=0)


def pick(bit, first, second):
    return jnp.where(bit == 0, first, second), jnp.where(bit == 0, second, first)


def solution(mesh):
    axis_name = mesh.axis_names[0]
    group_size = mesh.shape[axis_name]
    sharded = P(axis_name)
    in_specs = (sharded, sharded, sharded, sharded, sharded, P(), P()) + (sharded,) * 7
    out_specs = (sharded, sharded, sharded, sharded, P(), P()) + (sharded,) * 7
    CORE, XDIR, YDIR = 1, 2, 4

    def swap(value, mask):
        return lax.ppermute(value, axis_name, [(j, j ^ mask) for j in range(group_size)])

    def gather_rows(row_shard):
        return lax.all_gather(row_shard, axis_name, axis=0, tiled=True)

    def device_step(hidden, grad_out, positions, norm1_gain, norm2_gain, q_norm_gain, k_norm_gain, w_q, w_k, w_v, w_o, w_gate, w_up, w_down):
        batch_local, seq_len, width = hidden.shape
        tokens = batch_local * seq_len
        me = lax.axis_index(axis_name)
        c_bit, x_bit, y_bit = me % 2, (me // 2) % 2, me // 4
        ff_block = w_down.shape[0]
        rows = w_gate.shape[0]

        def row_tokens(own):
            far = swap(own, XDIR)
            near = jnp.concatenate([own, swap(own, CORE)], axis=0)
            return near, jnp.concatenate([far, swap(far, CORE)], axis=0)

        def quarter_columns(shard):
            blk = [shard[:, j * ff_block:(j + 1) * ff_block] for j in range(8)]
            first = jnp.concatenate([blk[0], blk[1], blk[4], blk[5]], axis=1)
            second = jnp.concatenate([blk[2], blk[3], blk[6], blk[7]], axis=1)
            keep, send = pick(x_bit, first, second)
            got = swap(send, XDIR)
            row0, row1 = pick(x_bit, keep, got)
            both = jnp.concatenate([row0, row1], axis=0)
            col = [both[:, j * ff_block:(j + 1) * ff_block] for j in range(4)]
            keep, send = pick(c_bit, jnp.concatenate([col[0], col[2]], axis=1), jnp.concatenate([col[1], col[3]], axis=1))
            got = swap(send, CORE)
            core0, core1 = pick(c_bit, keep, got)
            four = jnp.concatenate([core0[:rows], core1[:rows], core0[rows:], core1[rows:]], axis=0)
            got = swap(four, YDIR)
            return jnp.concatenate(pick(y_bit, four, got), axis=0)

        def far_sum(partial_rows):
            part = partial_rows(1, tokens, 2 * tokens)
            part = swap(part, CORE)
            return partial_rows(1, 0, tokens) + part

        def near_sum(partial_rows):
            part = partial_rows(0, tokens, 2 * tokens)
            part = swap(part, CORE)
            return partial_rows(0, 0, tokens) + part

        def token_product(left, right):
            return matmul_tn(left[0], right[0]) + matmul_tn(left[1], right[1])

        def scatter_columns(left_send, left_keep, right):
            part = token_product(left_send, right)
            got = swap(part, YDIR)
            mine = token_product(left_keep, right) + got
            blk = [mine[j * rows:(j + 1) * rows] for j in range(4)]
            keep, send = pick(c_bit, jnp.concatenate([blk[0], blk[2]], axis=0), jnp.concatenate([blk[1], blk[3]], axis=0))
            got = swap(send, CORE)
            core0, core1 = pick(c_bit, keep, got)
            both = jnp.concatenate([core0, core1], axis=1)
            keep, send = pick(x_bit, both[:rows], both[rows:])
            got = swap(send, XDIR)
            x0, x1 = pick(x_bit, keep, got)
            parts = [x0[:, :ff_block], x0[:, 2 * ff_block:3 * ff_block], x1[:, :ff_block], x1[:, 2 * ff_block:3 * ff_block]]
            parts += [x0[:, ff_block:2 * ff_block], x0[:, 3 * ff_block:], x1[:, ff_block:2 * ff_block], x1[:, 3 * ff_block:]]
            return jnp.concatenate(parts, axis=1)

        gains = lax.all_gather(jnp.stack([norm1_gain, norm2_gain]), axis_name, axis=1, tiled=True)
        full_q, full_k, full_v, full_o = gather_rows(w_q), gather_rows(w_k), gather_rows(w_v), gather_rows(w_o)
        gate_own, gains = lax.optimization_barrier((w_gate, gains))
        gain1, gain2 = gains[0].astype(jnp.float32), gains[1].astype(jnp.float32)
        up_own, full_k = lax.optimization_barrier((w_up, full_k))
        dy_flat = grad_out.reshape(tokens, width)
        dy_own, down_own, full_q = lax.optimization_barrier((dy_flat, w_down, full_q))
        gate_q = quarter_columns(gate_own)
        up_q = quarter_columns(up_own)
        down_q = jnp.concatenate(pick(y_bit, down_own, swap(down_own, YDIR)), axis=0)
        dy_row = row_tokens(dy_own)

        x_float = hidden.reshape(tokens, width).astype(jnp.float32)
        x_scale = rms_scale(x_float)
        x_unit = x_float * x_scale
        normed = (x_unit * gain1).astype(jnp.bfloat16)
        k_proj = matmul(normed, full_k).astype(jnp.bfloat16)
        v_proj = matmul(normed, full_v).astype(jnp.bfloat16)
        q_proj = matmul(normed, full_q).astype(jnp.bfloat16)
        head_dim = q_norm_gain.shape[0]
        cos_t, sin_t = rope_tables(positions, head_dim)
        attn_in = (q_proj, k_proj, v_proj, cos_t, sin_t, q_norm_gain.reshape(1, head_dim), k_norm_gain.reshape(1, head_dim))
        attn_ctx = attention_forward(attn_in, seq_len)
        attn_out = matmul(attn_ctx, full_o).astype(jnp.bfloat16)
        resid_float = (x_float + attn_out.astype(jnp.float32)).astype(jnp.bfloat16).astype(jnp.float32)
        r_scale = rms_scale(resid_float)
        r_unit = resid_float * r_scale
        mlp_in = row_tokens((r_unit * gain2).astype(jnp.bfloat16))

        acts, d_gates, d_ups = [], [], []
        inv_tokens = 1.0 / (tokens * group_size)
        for part in range(2):
            gate_float = matmul(mlp_in[part], gate_q).astype(jnp.bfloat16).astype(jnp.float32)
            up_float = matmul(mlp_in[part], up_q).astype(jnp.bfloat16).astype(jnp.float32)
            acts.append((jax.nn.silu(gate_float) * up_float).astype(jnp.bfloat16))
            dy_part = dy_row[part]
            if part:
                act_keep, act_send = zip(*(pick(y_bit, act[:, :ff_block], act[:, ff_block:]) for act in acts))
                down_part = token_product(act_send, dy_row)
                down_part, dy_part = lax.optimization_barrier((down_part, dy_part))
                down_got = swap(down_part, YDIR)
            d_mlp_act = matmul_nt(dy_part, down_q)
            gate_sig = jax.nn.sigmoid(gate_float)
            d_ups.append((d_mlp_act * gate_float * gate_sig).astype(jnp.bfloat16))
            d_gates.append((d_mlp_act * up_float * gate_sig * (1.0 + gate_float * (1.0 - gate_sig))).astype(jnp.bfloat16))

        def out_rows(far, lo, hi):
            return matmul(acts[far][lo:hi], down_q)

        def in_rows(far, lo, hi):
            return matmul_nt(d_gates[far][lo:hi], gate_q) + matmul_nt(d_ups[far][lo:hi], up_q)

        half = tokens // 2
        out_side = far_sum(out_rows)
        out_xa = swap(out_side[:half], XDIR)
        in_side = far_sum(in_rows)
        in_x = swap(in_side, XDIR)
        out_xb = swap(out_side[half:], XDIR)
        d_mlp_in = near_sum(in_rows) + in_x

        in_keep, in_send = zip(*(pick(y_bit, part[:, :width // 2], part[:, width // 2:]) for part in mlp_in))
        grad_gate = scatter_columns(in_send, in_keep, d_gates) * inv_tokens
        grad_up = scatter_columns(in_send, in_keep, d_ups) * inv_tokens
        grad_down = (token_product(act_keep, dy_row) + down_got) * inv_tokens
        down_total = near_sum(out_rows)

        grad_norm2 = jnp.sum(d_mlp_in * r_unit, axis=0)
        d_resid = dy_flat.astype(jnp.float32) + norm_backward(d_mlp_in * gain2, r_unit, r_scale)
        d_resid_bf = d_resid.astype(jnp.bfloat16)
        d_attn_ctx = matmul_nt(d_resid_bf, full_o).astype(jnp.bfloat16)
        out_xa, out_xb, _ = lax.optimization_barrier((out_xa, out_xb, d_attn_ctx))
        down_proj = (down_total + jnp.concatenate([out_xa, out_xb], axis=0)).astype(jnp.bfloat16)
        layer_out = (resid_float + down_proj.astype(jnp.float32)).astype(jnp.bfloat16).reshape(hidden.shape)
        wo_part = matmul_tn(attn_ctx, d_resid_bf) * inv_tokens
        wo_part, d_attn_ctx = lax.optimization_barrier((wo_part, d_attn_ctx))
        grad_wo = lax.psum_scatter(wo_part, axis_name, scatter_dimension=0, tiled=True)
        d_query, d_key, d_value, grad_qgain, grad_kgain = attention_backward(d_attn_ctx, attn_in, seq_len)
        wv_part = matmul_tn(normed, d_value) * inv_tokens
        grad_wv = lax.psum_scatter(wv_part, axis_name, scatter_dimension=0, tiled=True)
        wk_part = matmul_tn(normed, d_key) * inv_tokens
        grad_wk = lax.psum_scatter(wk_part, axis_name, scatter_dimension=0, tiled=True)
        wq_part = matmul_tn(normed, d_query) * inv_tokens
        grad_wq = lax.psum_scatter(wq_part, axis_name, scatter_dimension=0, tiled=True)
        d_normed = matmul_nt(d_query, full_q) + matmul_nt(d_key, full_k) + matmul_nt(d_value, full_v)
        grad_norm1 = jnp.sum(d_normed * x_unit, axis=0)
        d_hidden = (d_resid + norm_backward(d_normed * gain1, x_unit, x_scale)).astype(jnp.bfloat16).reshape(hidden.shape)

        small = jnp.concatenate([grad_norm1, grad_norm2, grad_qgain, grad_kgain]) * inv_tokens
        for mask in (CORE, XDIR, YDIR):
            small = small + swap(small, mask)
        own1 = lax.dynamic_slice_in_dim(small, me * rows, rows)
        own2 = lax.dynamic_slice_in_dim(small, width + me * rows, rows)
        gq = small[2 * width:2 * width + head_dim]
        gk = small[2 * width + head_dim:]
        return (layer_out, d_hidden, own1, own2, gq, gk, grad_wq, grad_wk, grad_wv, grad_wo, grad_gate, grad_up, grad_down)

    return jax.shard_map(device_step, mesh=mesh, in_specs=in_specs, out_specs=out_specs, check_vma=False)
```

```python
import jax
import jax.numpy as jnp
from jax import lax
from jax.experimental import pallas as pl
from jax.experimental.pallas import tpu as pltpu
from jax.sharding import PartitionSpec as P


RMS_EPS = 1e-6
ROPE_THETA = 1000000.0
NEG = -1e30


def rms_scale(tensor):
    return lax.rsqrt(jnp.mean(tensor * tensor, axis=-1, keepdims=True) + RMS_EPS)


def norm_backward(d_unit, unit_val, scale_val):
    return scale_val * (d_unit - unit_val * jnp.mean(d_unit * unit_val, axis=-1, keepdims=True))


def matmul(left_op, right_op):
    return jnp.dot(left_op, right_op, preferred_element_type=jnp.float32)


def matmul_tn(left_op, right_op):
    return lax.dot_general(left_op, right_op, (((0,), (0,)), ((), ())), preferred_element_type=jnp.float32)


def matmul_nt(left_op, right_op):
    return lax.dot_general(left_op, right_op, (((1,), (1,)), ((), ())), preferred_element_type=jnp.float32)


def rope_tables(positions, head_dim):
    inv_freq = ROPE_THETA ** (-2.0 * jnp.arange(head_dim // 2, dtype=jnp.float32) / head_dim)
    rope_angle = positions.reshape(-1, 1).astype(jnp.float32) * inv_freq
    cos_half = jnp.cos(rope_angle)
    sin_half = jnp.sin(rope_angle)
    return jnp.concatenate([cos_half, cos_half], axis=-1), jnp.concatenate([-sin_half, sin_half], axis=-1)


def half_turn(tensor):
    return pltpu.roll(tensor, tensor.shape[-1] // 2, 1)


def head_unit(projected):
    heads = projected.astype(jnp.float32)
    scale = rms_scale(heads)
    return heads * scale, scale


def head_rope(unit, gain, cos_t, sin_t):
    scaled = unit * gain
    return (scaled * cos_t + half_turn(scaled) * sin_t).astype(jnp.bfloat16)


def head_backward(d_rot, unit, scale, gain, cos_t, sin_t):
    d_scaled = d_rot * cos_t + half_turn(d_rot * sin_t)
    d_gain = jnp.sum((d_scaled * unit).reshape(-1, 8, d_rot.shape[-1]), axis=0)
    return norm_backward(d_scaled * gain, unit, scale).astype(jnp.bfloat16), d_gain


def head_probs(q_rot, k_rot):
    seq_len, head_dim = q_rot.shape
    scores = matmul_nt(q_rot, k_rot) * (head_dim ** -0.5)
    query = lax.broadcasted_iota(jnp.int32, (seq_len, seq_len), 0)
    key = lax.broadcasted_iota(jnp.int32, (seq_len, seq_len), 1)
    scores = jnp.where(query >= key, scores, NEG)
    weight = jnp.exp(scores - jnp.max(scores, axis=-1, keepdims=True))
    return weight / jnp.sum(weight, axis=-1, keepdims=True)


def attention_forward_kernel(q_ref, k_ref, v_ref, cos_ref, sin_ref, qg_ref, kg_ref, ctx_ref):
    head_dim = k_ref.shape[1]
    cos_t, sin_t = cos_ref[...], sin_ref[...]
    q_gain, k_gain = qg_ref[...].astype(jnp.float32), kg_ref[...].astype(jnp.float32)
    k_rot = head_rope(head_unit(k_ref[...])[0], k_gain, cos_t, sin_t)
    for g in range(q_ref.shape[1] // head_dim):
        cols = slice(g * head_dim, (g + 1) * head_dim)
        q_rot = head_rope(head_unit(q_ref[:, cols])[0], q_gain, cos_t, sin_t)
        probs = head_probs(q_rot, k_rot).astype(jnp.bfloat16)
        ctx_ref[:, cols] = matmul(probs, v_ref[...]).astype(jnp.bfloat16)


def attention_backward_kernel(d_ref, q_ref, k_ref, v_ref, cos_ref, sin_ref, qg_ref, kg_ref, dq_ref, dk_ref, dv_ref, dqg_ref, dkg_ref):
    head_dim = k_ref.shape[1]
    cos_t, sin_t = cos_ref[...], sin_ref[...]
    q_gain, k_gain = qg_ref[...].astype(jnp.float32), kg_ref[...].astype(jnp.float32)
    k_unit, k_scale = head_unit(k_ref[...])
    k_rot = head_rope(k_unit, k_gain, cos_t, sin_t)
    d_k_rot = d_value = d_q_gain = 0.0
    for g in range(q_ref.shape[1] // head_dim):
        cols = slice(g * head_dim, (g + 1) * head_dim)
        q_unit, q_scale = head_unit(q_ref[:, cols])
        q_rot = head_rope(q_unit, q_gain, cos_t, sin_t)
        probs = head_probs(q_rot, k_rot)
        d_ctx = d_ref[:, cols]
        d_value = d_value + matmul_tn(probs.astype(jnp.bfloat16), d_ctx)
        d_probs = matmul_nt(d_ctx, v_ref[...])
        d_scores = probs * (d_probs - jnp.sum(probs * d_probs, axis=-1, keepdims=True))
        d_scores = (d_scores * (head_dim ** -0.5)).astype(jnp.bfloat16)
        d_k_rot = d_k_rot + matmul_tn(d_scores, q_rot)
        dq_ref[:, cols], part = head_backward(matmul(d_scores, k_rot), q_unit, q_scale, q_gain, cos_t, sin_t)
        d_q_gain = d_q_gain + part
    dqg_ref[...] = d_q_gain
    dk_ref[...], dkg_ref[...] = head_backward(d_k_rot, k_unit, k_scale, k_gain, cos_t, sin_t)
    dv_ref[...] = d_value.astype(jnp.bfloat16)


def attention_specs(qkv, heads, kv_heads, seq_len, head_dim):
    q_spec = pl.BlockSpec((seq_len, heads // kv_heads * head_dim), lambda b, h: (b, h))
    k_spec = pl.BlockSpec((seq_len, head_dim), lambda b, h: (b, heads + h))
    v_spec = pl.BlockSpec((seq_len, head_dim), lambda b, h: (b, heads + kv_heads + h))
    t_spec = pl.BlockSpec((seq_len, head_dim), lambda b, h: (b, 0))
    g_spec = pl.BlockSpec((1, head_dim), lambda b, h: (0, 0))
    return (qkv.shape[0] // seq_len, kv_heads), q_spec, [q_spec, k_spec, v_spec, t_spec, t_spec, g_spec, g_spec]


def attention_forward(qkv, tables, heads, kv_heads, seq_len):
    head_dim = tables[0].shape[1]
    grid, q_spec, in_specs = attention_specs(qkv, heads, kv_heads, seq_len, head_dim)
    width = heads * head_dim
    return pl.pallas_call(
        attention_forward_kernel, grid=grid, in_specs=in_specs, out_specs=q_spec,
        out_shape=jax.ShapeDtypeStruct((qkv.shape[0], width), jnp.bfloat16),
        cost_estimate=pl.CostEstimate(flops=2 * qkv.size * seq_len, bytes_accessed=3 * qkv.size, transcendentals=0),
        name="attn_fwd",
    )(qkv, qkv, qkv, *tables)


def attention_backward(d_ctx, qkv, tables, heads, kv_heads, seq_len):
    head_dim = tables[0].shape[1]
    grid, q_spec, in_specs = attention_specs(qkv, heads, kv_heads, seq_len, head_dim)
    k_spec = pl.BlockSpec((seq_len, head_dim), lambda b, h: (b, h))
    k_shape = jax.ShapeDtypeStruct((qkv.shape[0], kv_heads * head_dim), jnp.bfloat16)
    gain_spec = pl.BlockSpec((8, head_dim), lambda b, h: (b * grid[1] + h, 0))
    gain_shape = jax.ShapeDtypeStruct((8 * grid[0] * grid[1], head_dim), jnp.float32)
    dq, dk, dv, dqg, dkg = pl.pallas_call(
        attention_backward_kernel, grid=grid, in_specs=[q_spec] + in_specs,
        out_specs=[q_spec, k_spec, k_spec, gain_spec, gain_spec],
        out_shape=[jax.ShapeDtypeStruct(d_ctx.shape, jnp.bfloat16), k_shape, k_shape, gain_shape, gain_shape],
        cost_estimate=pl.CostEstimate(flops=5 * qkv.size * seq_len, bytes_accessed=6 * qkv.size, transcendentals=0),
        name="attn_bwd",
    )(d_ctx, qkv, qkv, qkv, *tables)
    return jnp.concatenate([dq, dk, dv], axis=1), jnp.sum(dqg, axis=0), jnp.sum(dkg, axis=0)


def pick(bit, first, second):
    return jnp.where(bit == 0, first, second), jnp.where(bit == 0, second, first)


def solution(mesh):
    axis_name = mesh.axis_names[0]
    group_size = mesh.shape[axis_name]
    sharded = P(axis_name)
    in_specs = (sharded, sharded, sharded, sharded, sharded, P(), P()) + (sharded,) * 7
    out_specs = (sharded, sharded, sharded, sharded, P(), P()) + (sharded,) * 7
    CORE, XDIR, YDIR = 1, 2, 4

    def swap(value, mask):
        return lax.ppermute(value, axis_name, [(j, j ^ mask) for j in range(group_size)])

    def gather_rows(row_shard):
        return lax.all_gather(row_shard, axis_name, axis=0, tiled=True)

    def device_step(hidden, grad_out, positions, norm1_gain, norm2_gain, q_norm_gain, k_norm_gain, w_q, w_k, w_v, w_o, w_gate, w_up, w_down):
        batch_local, seq_len, width = hidden.shape
        tokens = batch_local * seq_len
        me = lax.axis_index(axis_name)
        c_bit, x_bit, y_bit = me % 2, (me // 2) % 2, me // 4
        ff_block = w_down.shape[0]
        rows = w_gate.shape[0]

        def row_tokens(own):
            far = swap(own, XDIR)
            near = jnp.concatenate([own, swap(own, CORE)], axis=0)
            return near, jnp.concatenate([far, swap(far, CORE)], axis=0)

        def quarter_columns(shard):
            blk = [shard[:, j * ff_block:(j + 1) * ff_block] for j in range(8)]
            first = jnp.concatenate([blk[0], blk[1], blk[4], blk[5]], axis=1)
            second = jnp.concatenate([blk[2], blk[3], blk[6], blk[7]], axis=1)
            keep, send = pick(x_bit, first, second)
            first = got = swap(send, XDIR)
            row0, row1 = pick(x_bit, keep, got)
            both = jnp.concatenate([row0, row1], axis=0)
            col = [both[:, j * ff_block:(j + 1) * ff_block] for j in range(4)]
            keep, send = pick(c_bit, jnp.concatenate([col[0], col[2]], axis=1), jnp.concatenate([col[1], col[3]], axis=1))
            got = swap(send, CORE)
            core0, core1 = pick(c_bit, keep, got)
            four = jnp.concatenate([core0[:rows], core1[:rows], core0[rows:], core1[rows:]], axis=0)
            got = swap(four, YDIR)
            return jnp.concatenate(pick(y_bit, four, got), axis=0), first

        def far_sum(add_rows):
            part = add_rows(None, 1, tokens, 2 * tokens)
            part = swap(part, CORE)
            return add_rows(part, 1, 0, tokens)

        def near_sum(add_rows):
            part = add_rows(None, 0, tokens, 2 * tokens)
            part = swap(part, CORE)
            return add_rows(part, 0, 0, tokens)

        def plus(base, product):
            return product if base is None else base + product

        def token_product(left, right, base=None):
            return plus(plus(base, matmul_tn(left[0], right[0])), matmul_tn(left[1], right[1]))

        def scatter_columns(left_send, left_keep, right):
            part = token_product(left_send, right)
            got = swap(part, YDIR)
            mine = token_product(left_keep, right, got)
            blk = [mine[j * rows:(j + 1) * rows] for j in range(4)]
            keep, send = pick(c_bit, jnp.concatenate([blk[0], blk[2]], axis=0), jnp.concatenate([blk[1], blk[3]], axis=0))
            got = swap(send, CORE)
            core0, core1 = pick(c_bit, keep, got)
            both = jnp.concatenate([core0, core1], axis=1)
            keep, send = pick(x_bit, both[:rows], both[rows:])
            got = swap(send, XDIR)
            x0, x1 = pick(x_bit, keep, got)
            parts = [x0[:, :ff_block], x0[:, 2 * ff_block:3 * ff_block], x1[:, :ff_block], x1[:, 2 * ff_block:3 * ff_block]]
            parts += [x0[:, ff_block:2 * ff_block], x0[:, 3 * ff_block:], x1[:, ff_block:2 * ff_block], x1[:, 3 * ff_block:]]
            return jnp.concatenate(parts, axis=1)

        gains = lax.all_gather(jnp.stack([norm1_gain, norm2_gain]), axis_name, axis=1, tiled=True)
        full_qkv, full_o = gather_rows(jnp.concatenate([w_q, w_k, w_v], axis=1)), gather_rows(w_o)
        gate_own, down_own, gains = lax.optimization_barrier((w_gate, w_down, gains))
        gain1, gain2 = gains[0].astype(jnp.float32), gains[1].astype(jnp.float32)
        dy_flat = grad_out.reshape(tokens, width)
        dy_own, full_qkv = lax.optimization_barrier((dy_flat, full_qkv))
        gate_q, gate_first = quarter_columns(gate_own)
        up_own, _ = lax.optimization_barrier((w_up, gate_first))
        up_q, _ = quarter_columns(up_own)
        down_q = jnp.concatenate(pick(y_bit, down_own, swap(down_own, YDIR)), axis=0)
        dy_row = row_tokens(dy_own)

        x_float = hidden.reshape(tokens, width).astype(jnp.float32)
        x_scale = rms_scale(x_float)
        x_unit = x_float * x_scale
        normed = (x_unit * gain1).astype(jnp.bfloat16)
        qkv = matmul(normed, full_qkv).astype(jnp.bfloat16)
        head_dim = q_norm_gain.shape[0]
        heads, kv_heads = w_q.shape[1] // head_dim, w_k.shape[1] // head_dim
        tables = rope_tables(positions, head_dim) + (q_norm_gain.reshape(1, head_dim), k_norm_gain.reshape(1, head_dim))
        attn_ctx = attention_forward(qkv, tables, heads, kv_heads, seq_len)
        attn_out = matmul(attn_ctx, full_o).astype(jnp.bfloat16)
        resid_float = (x_float + attn_out.astype(jnp.float32)).astype(jnp.bfloat16).astype(jnp.float32)
        r_scale = rms_scale(resid_float)
        r_unit = resid_float * r_scale
        mlp_in = row_tokens((r_unit * gain2).astype(jnp.bfloat16))

        acts, d_gates, d_ups = [], [], []
        inv_tokens = 1.0 / (tokens * group_size)
        for part in range(2):
            gate_float = matmul(mlp_in[part], gate_q).astype(jnp.bfloat16).astype(jnp.float32)
            up_float = matmul(mlp_in[part], up_q).astype(jnp.bfloat16).astype(jnp.float32)
            acts.append((jax.nn.silu(gate_float) * up_float).astype(jnp.bfloat16))
            dy_part = dy_row[part]
            if part:
                act_keep, act_send = zip(*(pick(y_bit, act[:, :ff_block], act[:, ff_block:]) for act in acts))
                down_part = token_product(act_send, dy_row)
                down_part, dy_part = lax.optimization_barrier((down_part, dy_part))
                down_got = swap(down_part, YDIR)
            d_mlp_act = matmul_nt(dy_part, down_q)
            gate_sig = jax.nn.sigmoid(gate_float)
            d_ups.append((d_mlp_act * gate_float * gate_sig).astype(jnp.bfloat16))
            d_gates.append((d_mlp_act * up_float * gate_sig * (1.0 + gate_float * (1.0 - gate_sig))).astype(jnp.bfloat16))

        def out_rows(base, far, lo, hi):
            return plus(base, matmul(acts[far][lo:hi], down_q))

        def in_rows(base, far, lo, hi):
            return plus(plus(base, matmul_nt(d_gates[far][lo:hi], gate_q)), matmul_nt(d_ups[far][lo:hi], up_q))

        half = tokens // 2
        out_side = far_sum(out_rows)
        out_xa = swap(out_side[:half], XDIR)
        in_side = far_sum(in_rows)
        in_x = swap(in_side, XDIR)
        out_xb = swap(out_side[half:], XDIR)
        d_mlp_in = near_sum(in_rows) + in_x

        in_keep, in_send = zip(*(pick(y_bit, part[:, :width // 2], part[:, width // 2:]) for part in mlp_in))
        grad_gate = scatter_columns(in_send, in_keep, d_gates) * inv_tokens
        grad_up = scatter_columns(in_send, in_keep, d_ups) * inv_tokens
        grad_down = token_product(act_keep, dy_row, down_got) * inv_tokens
        down_total = near_sum(out_rows)

        grad_norm2 = jnp.sum(d_mlp_in * r_unit, axis=0)
        d_resid = dy_flat.astype(jnp.float32) + norm_backward(d_mlp_in * gain2, r_unit, r_scale)
        d_resid_bf = d_resid.astype(jnp.bfloat16)
        d_attn_ctx = matmul_nt(d_resid_bf, full_o).astype(jnp.bfloat16)
        out_xa, out_xb, _ = lax.optimization_barrier((out_xa, out_xb, d_attn_ctx))
        down_proj = (down_total + jnp.concatenate([out_xa, out_xb], axis=0)).astype(jnp.bfloat16)
        layer_out = (resid_float + down_proj.astype(jnp.float32)).astype(jnp.bfloat16).reshape(hidden.shape)
        wo_part = matmul_tn(attn_ctx, d_resid_bf) * inv_tokens
        wo_part, d_attn_ctx = lax.optimization_barrier((wo_part, d_attn_ctx))
        grad_wo = lax.psum_scatter(wo_part, axis_name, scatter_dimension=0, tiled=True)
        d_qkv, grad_qgain, grad_kgain = attention_backward(d_attn_ctx, qkv, tables, heads, kv_heads, seq_len)
        qkv_part = matmul_tn(normed, d_qkv) * inv_tokens
        grad_qkv = lax.psum_scatter(qkv_part, axis_name, scatter_dimension=0, tiled=True)
        grad_wq, grad_wk, grad_wv = jnp.split(grad_qkv, (w_q.shape[1], w_q.shape[1] + w_k.shape[1]), axis=1)
        d_normed = matmul_nt(d_qkv, full_qkv)
        grad_norm1 = jnp.sum(d_normed * x_unit, axis=0)
        d_hidden = (d_resid + norm_backward(d_normed * gain1, x_unit, x_scale)).astype(jnp.bfloat16).reshape(hidden.shape)

        small = jnp.concatenate([grad_norm1, grad_norm2, grad_qgain, grad_kgain]) * inv_tokens
        for mask in (CORE, XDIR, YDIR):
            small = small + swap(small, mask)
        own1 = lax.dynamic_slice_in_dim(small, me * rows, rows)
        own2 = lax.dynamic_slice_in_dim(small, width + me * rows, rows)
        gq = small[2 * width:2 * width + head_dim]
        gk = small[2 * width + head_dim:]
        return (layer_out, d_hidden, own1, own2, gq, gk, grad_wq, grad_wk, grad_wv, grad_wo, grad_gate, grad_up, grad_down)

    return jax.shard_map(device_step, mesh=mesh, in_specs=in_specs, out_specs=out_specs, check_vma=False)
```

```python
import jax
import jax.numpy as jnp
from jax import lax
from jax.experimental import pallas as pl
from jax.experimental.pallas import tpu as pltpu
from jax.sharding import PartitionSpec as P


RMS_EPS = 1e-6
ROPE_THETA = 1000000.0
NEG = -1e30


def rms_scale(tensor):
    return lax.rsqrt(jnp.mean(tensor * tensor, axis=-1, keepdims=True) + RMS_EPS)


def norm_backward(d_unit, unit_val, scale_val):
    return scale_val * (d_unit - unit_val * jnp.mean(d_unit * unit_val, axis=-1, keepdims=True))


def matmul(left_op, right_op):
    return jnp.dot(left_op, right_op, preferred_element_type=jnp.float32)


def matmul_tn(left_op, right_op):
    return lax.dot_general(left_op, right_op, (((0,), (0,)), ((), ())), preferred_element_type=jnp.float32)


def matmul_nt(left_op, right_op):
    return lax.dot_general(left_op, right_op, (((1,), (1,)), ((), ())), preferred_element_type=jnp.float32)


def rope_tables(positions, head_dim):
    inv_freq = ROPE_THETA ** (-2.0 * jnp.arange(head_dim // 2, dtype=jnp.float32) / head_dim)
    rope_angle = positions.reshape(-1, 1).astype(jnp.float32) * inv_freq
    cos_half = jnp.cos(rope_angle)
    sin_half = jnp.sin(rope_angle)
    return jnp.concatenate([cos_half, cos_half], axis=-1), jnp.concatenate([-sin_half, sin_half], axis=-1)


def half_turn(tensor):
    return pltpu.roll(tensor, tensor.shape[-1] // 2, 1)


def head_unit(projected):
    heads = projected.astype(jnp.float32)
    scale = rms_scale(heads)
    return heads * scale, scale


def head_rope(unit, gain, cos_t, sin_t):
    scaled = unit * gain
    return (scaled * cos_t + half_turn(scaled) * sin_t).astype(jnp.bfloat16)


def head_backward(d_rot, unit, scale, gain, cos_t, sin_t):
    d_scaled = d_rot * cos_t + half_turn(d_rot * sin_t)
    d_gain = jnp.sum((d_scaled * unit).reshape(-1, 8, d_rot.shape[-1]), axis=0)
    return norm_backward(d_scaled * gain, unit, scale).astype(jnp.bfloat16), d_gain


def head_probs(q_rot, k_rot):
    seq_len, head_dim = q_rot.shape
    scores = matmul_nt(q_rot, k_rot) * (head_dim ** -0.5)
    query = lax.broadcasted_iota(jnp.int32, (seq_len, seq_len), 0)
    key = lax.broadcasted_iota(jnp.int32, (seq_len, seq_len), 1)
    scores = jnp.where(query >= key, scores, NEG)
    weight = jnp.exp(scores - jnp.max(scores, axis=-1, keepdims=True))
    return weight / jnp.sum(weight, axis=-1, keepdims=True)


def attention_forward_kernel(q_ref, k_ref, v_ref, cos_ref, sin_ref, qg_ref, kg_ref, ctx_ref):
    head_dim = k_ref.shape[1]
    cos_t, sin_t = cos_ref[...], sin_ref[...]
    q_gain, k_gain = qg_ref[...].astype(jnp.float32), kg_ref[...].astype(jnp.float32)
    k_rot = head_rope(head_unit(k_ref[...])[0], k_gain, cos_t, sin_t)
    for g in range(q_ref.shape[1] // head_dim):
        cols = slice(g * head_dim, (g + 1) * head_dim)
        q_rot = head_rope(head_unit(q_ref[:, cols])[0], q_gain, cos_t, sin_t)
        probs = head_probs(q_rot, k_rot).astype(jnp.bfloat16)
        ctx_ref[:, cols] = matmul(probs, v_ref[...]).astype(jnp.bfloat16)


def attention_backward_kernel(d_ref, q_ref, k_ref, v_ref, cos_ref, sin_ref, qg_ref, kg_ref, dq_ref, dk_ref, dv_ref, dqg_ref, dkg_ref):
    head_dim = k_ref.shape[1]
    cos_t, sin_t = cos_ref[...], sin_ref[...]
    q_gain, k_gain = qg_ref[...].astype(jnp.float32), kg_ref[...].astype(jnp.float32)
    k_unit, k_scale = head_unit(k_ref[...])
    k_rot = head_rope(k_unit, k_gain, cos_t, sin_t)
    d_k_rot = d_value = d_q_gain = 0.0
    for g in range(q_ref.shape[1] // head_dim):
        cols = slice(g * head_dim, (g + 1) * head_dim)
        q_unit, q_scale = head_unit(q_ref[:, cols])
        q_rot = head_rope(q_unit, q_gain, cos_t, sin_t)
        probs = head_probs(q_rot, k_rot)
        d_ctx = d_ref[:, cols]
        d_value = d_value + matmul_tn(probs.astype(jnp.bfloat16), d_ctx)
        d_probs = matmul_nt(d_ctx, v_ref[...])
        d_scores = probs * (d_probs - jnp.sum(probs * d_probs, axis=-1, keepdims=True))
        d_scores = (d_scores * (head_dim ** -0.5)).astype(jnp.bfloat16)
        d_k_rot = d_k_rot + matmul_tn(d_scores, q_rot)
        dq_ref[:, cols], part = head_backward(matmul(d_scores, k_rot), q_unit, q_scale, q_gain, cos_t, sin_t)
        d_q_gain = d_q_gain + part
    dqg_ref[...] = d_q_gain
    dk_ref[...], dkg_ref[...] = head_backward(d_k_rot, k_unit, k_scale, k_gain, cos_t, sin_t)
    dv_ref[...] = d_value.astype(jnp.bfloat16)


def attention_specs(qkv, heads, kv_heads, seq_len, head_dim):
    q_spec = pl.BlockSpec((seq_len, heads // kv_heads * head_dim), lambda b, h: (b, h))
    k_spec = pl.BlockSpec((seq_len, head_dim), lambda b, h: (b, heads + h))
    v_spec = pl.BlockSpec((seq_len, head_dim), lambda b, h: (b, heads + kv_heads + h))
    t_spec = pl.BlockSpec((seq_len, head_dim), lambda b, h: (b, 0))
    g_spec = pl.BlockSpec((1, head_dim), lambda b, h: (0, 0))
    return (qkv.shape[0] // seq_len, kv_heads), q_spec, [q_spec, k_spec, v_spec, t_spec, t_spec, g_spec, g_spec]


def attention_forward(qkv, tables, heads, kv_heads, seq_len):
    head_dim = tables[0].shape[1]
    grid, q_spec, in_specs = attention_specs(qkv, heads, kv_heads, seq_len, head_dim)
    width = heads * head_dim
    return pl.pallas_call(
        attention_forward_kernel, grid=grid, in_specs=in_specs, out_specs=q_spec,
        out_shape=jax.ShapeDtypeStruct((qkv.shape[0], width), jnp.bfloat16),
        cost_estimate=pl.CostEstimate(flops=2 * qkv.size * seq_len, bytes_accessed=3 * qkv.size, transcendentals=0),
        name="attn_fwd",
    )(qkv, qkv, qkv, *tables)


def attention_backward(d_ctx, qkv, tables, heads, kv_heads, seq_len):
    head_dim = tables[0].shape[1]
    grid, q_spec, in_specs = attention_specs(qkv, heads, kv_heads, seq_len, head_dim)
    k_spec = pl.BlockSpec((seq_len, head_dim), lambda b, h: (b, h))
    k_shape = jax.ShapeDtypeStruct((qkv.shape[0], kv_heads * head_dim), jnp.bfloat16)
    gain_spec = pl.BlockSpec((8, head_dim), lambda b, h: (b * grid[1] + h, 0))
    gain_shape = jax.ShapeDtypeStruct((8 * grid[0] * grid[1], head_dim), jnp.float32)
    dq, dk, dv, dqg, dkg = pl.pallas_call(
        attention_backward_kernel, grid=grid, in_specs=[q_spec] + in_specs,
        out_specs=[q_spec, k_spec, k_spec, gain_spec, gain_spec],
        out_shape=[jax.ShapeDtypeStruct(d_ctx.shape, jnp.bfloat16), k_shape, k_shape, gain_shape, gain_shape],
        cost_estimate=pl.CostEstimate(flops=5 * qkv.size * seq_len, bytes_accessed=6 * qkv.size, transcendentals=0),
        name="attn_bwd",
    )(d_ctx, qkv, qkv, qkv, *tables)
    return jnp.concatenate([dq, dk, dv], axis=1), jnp.sum(dqg, axis=0), jnp.sum(dkg, axis=0)


def pick(bit, first, second):
    return jnp.where(bit == 0, first, second), jnp.where(bit == 0, second, first)


def solution(mesh):
    axis_name = mesh.axis_names[0]
    group_size = mesh.shape[axis_name]
    sharded = P(axis_name)
    in_specs = (sharded, sharded, sharded, sharded, sharded, P(), P()) + (sharded,) * 7
    out_specs = (sharded, sharded, sharded, sharded, P(), P()) + (sharded,) * 7
    CORE, XDIR, YDIR = 1, 2, 4

    def swap(value, mask):
        return lax.ppermute(value, axis_name, [(j, j ^ mask) for j in range(group_size)])

    def gather_rows(row_shard):
        return lax.all_gather(row_shard, axis_name, axis=0, tiled=True)

    def device_step(hidden, grad_out, positions, norm1_gain, norm2_gain, q_norm_gain, k_norm_gain, w_q, w_k, w_v, w_o, w_gate, w_up, w_down):
        batch_local, seq_len, width = hidden.shape
        tokens = batch_local * seq_len
        me = lax.axis_index(axis_name)
        c_bit, x_bit, y_bit = me % 2, (me // 2) % 2, me // 4
        ff_block = w_down.shape[0]
        rows = w_gate.shape[0]

        def row_tokens(own):
            far = swap(own, XDIR)
            near = jnp.concatenate([own, swap(own, CORE)], axis=0)
            return near, jnp.concatenate([far, swap(far, CORE)], axis=0)

        def quarter_columns(shard):
            blk = [shard[:, j * ff_block:(j + 1) * ff_block] for j in range(8)]
            first = jnp.concatenate([blk[0], blk[1], blk[4], blk[5]], axis=1)
            second = jnp.concatenate([blk[2], blk[3], blk[6], blk[7]], axis=1)
            keep, send = pick(x_bit, first, second)
            got = swap(send, XDIR)
            row0, row1 = pick(x_bit, keep, got)
            both = jnp.concatenate([row0, row1], axis=0)
            col = [both[:, j * ff_block:(j + 1) * ff_block] for j in range(4)]
            keep, send = pick(c_bit, jnp.concatenate([col[0], col[2]], axis=1), jnp.concatenate([col[1], col[3]], axis=1))
            got = swap(send, CORE)
            core0, core1 = pick(c_bit, keep, got)
            four = jnp.concatenate([core0[:rows], core1[:rows], core0[rows:], core1[rows:]], axis=0)
            got = swap(four, YDIR)
            return jnp.concatenate(pick(y_bit, four, got), axis=0)

        def far_sum(add_rows):
            part = add_rows(None, 1, tokens, 2 * tokens)
            part = swap(part, CORE)
            return add_rows(part, 1, 0, tokens)

        def near_sum(add_rows):
            part = add_rows(None, 0, tokens, 2 * tokens)
            part = swap(part, CORE)
            return add_rows(part, 0, 0, tokens)

        def plus(base, product):
            return product if base is None else base + product

        def token_product(left, right, base=None):
            return plus(plus(base, matmul_tn(left[0], right[0])), matmul_tn(left[1], right[1]))

        def scatter_columns(left_send, left_keep, right):
            part = token_product(left_send, right)
            got = swap(part, YDIR)
            mine = token_product(left_keep, right, got)
            blk = [mine[j * rows:(j + 1) * rows] for j in range(4)]
            keep, send = pick(c_bit, jnp.concatenate([blk[0], blk[2]], axis=0), jnp.concatenate([blk[1], blk[3]], axis=0))
            got = swap(send, CORE)
            core0, core1 = pick(c_bit, keep, got)
            both = jnp.concatenate([core0, core1], axis=1)
            keep, send = pick(x_bit, both[:rows], both[rows:])
            got = swap(send, XDIR)
            x0, x1 = pick(x_bit, keep, got)
            parts = [x0[:, :ff_block], x0[:, 2 * ff_block:3 * ff_block], x1[:, :ff_block], x1[:, 2 * ff_block:3 * ff_block]]
            parts += [x0[:, ff_block:2 * ff_block], x0[:, 3 * ff_block:], x1[:, ff_block:2 * ff_block], x1[:, 3 * ff_block:]]
            return jnp.concatenate(parts, axis=1)

        gains = lax.all_gather(jnp.stack([norm1_gain, norm2_gain]), axis_name, axis=1, tiled=True)
        full_qkv, full_o = gather_rows(jnp.concatenate([w_q, w_k, w_v], axis=1)), gather_rows(w_o)
        gate_own, gains = lax.optimization_barrier((w_gate, gains))
        gain1, gain2 = gains[0].astype(jnp.float32), gains[1].astype(jnp.float32)
        dy_flat = grad_out.reshape(tokens, width)
        up_own, down_own, dy_own, full_qkv = lax.optimization_barrier((w_up, w_down, dy_flat, full_qkv))
        gate_q = quarter_columns(gate_own)
        up_q = quarter_columns(up_own)
        down_q = jnp.concatenate(pick(y_bit, down_own, swap(down_own, YDIR)), axis=0)
        dy_row = row_tokens(dy_own)

        x_float = hidden.reshape(tokens, width).astype(jnp.float32)
        x_scale = rms_scale(x_float)
        x_unit = x_float * x_scale
        normed = (x_unit * gain1).astype(jnp.bfloat16)
        qkv = matmul(normed, full_qkv).astype(jnp.bfloat16)
        head_dim = q_norm_gain.shape[0]
        heads, kv_heads = w_q.shape[1] // head_dim, w_k.shape[1] // head_dim
        tables = rope_tables(positions, head_dim) + (q_norm_gain.reshape(1, head_dim), k_norm_gain.reshape(1, head_dim))
        attn_ctx = attention_forward(qkv, tables, heads, kv_heads, seq_len)
        attn_out = matmul(attn_ctx, full_o).astype(jnp.bfloat16)
        resid_float = (x_float + attn_out.astype(jnp.float32)).astype(jnp.bfloat16).astype(jnp.float32)
        r_scale = rms_scale(resid_float)
        r_unit = resid_float * r_scale
        mlp_in = row_tokens((r_unit * gain2).astype(jnp.bfloat16))

        acts, d_gates, d_ups = [], [], []
        inv_tokens = 1.0 / (tokens * group_size)
        for part in range(2):
            gate_float = matmul(mlp_in[part], gate_q).astype(jnp.bfloat16).astype(jnp.float32)
            up_float = matmul(mlp_in[part], up_q).astype(jnp.bfloat16).astype(jnp.float32)
            acts.append((jax.nn.silu(gate_float) * up_float).astype(jnp.bfloat16))
            dy_part = dy_row[part]
            if part:
                act_keep, act_send = zip(*(pick(y_bit, act[:, :ff_block], act[:, ff_block:]) for act in acts))
                down_part = token_product(act_send, dy_row)
                down_part, dy_part = lax.optimization_barrier((down_part, dy_part))
                down_got = swap(down_part, YDIR)
            d_mlp_act = matmul_nt(dy_part, down_q)
            gate_sig = jax.nn.sigmoid(gate_float)
            d_ups.append((d_mlp_act * gate_float * gate_sig).astype(jnp.bfloat16))
            d_gates.append((d_mlp_act * up_float * gate_sig * (1.0 + gate_float * (1.0 - gate_sig))).astype(jnp.bfloat16))

        def out_rows(base, far, lo, hi):
            return plus(base, matmul(acts[far][lo:hi], down_q))

        def in_rows(base, far, lo, hi):
            return plus(plus(base, matmul_nt(d_gates[far][lo:hi], gate_q)), matmul_nt(d_ups[far][lo:hi], up_q))

        half = tokens // 2
        out_side = far_sum(out_rows)
        out_xa = swap(out_side[:half], XDIR)
        in_side = far_sum(in_rows)
        in_x = swap(in_side, XDIR)
        out_xb = swap(out_side[half:], XDIR)
        d_mlp_in = near_sum(in_rows) + in_x

        in_keep, in_send = zip(*(pick(y_bit, part[:, :width // 2], part[:, width // 2:]) for part in mlp_in))
        grad_gate = scatter_columns(in_send, in_keep, d_gates) * inv_tokens
        grad_up = scatter_columns(in_send, in_keep, d_ups) * inv_tokens
        grad_down = token_product(act_keep, dy_row, down_got) * inv_tokens
        down_total = near_sum(out_rows)

        grad_norm2 = jnp.sum(d_mlp_in * r_unit, axis=0)
        d_resid = dy_flat.astype(jnp.float32) + norm_backward(d_mlp_in * gain2, r_unit, r_scale)
        d_resid_bf = d_resid.astype(jnp.bfloat16)
        d_attn_ctx = matmul_nt(d_resid_bf, full_o).astype(jnp.bfloat16)
        out_xa, out_xb, _ = lax.optimization_barrier((out_xa, out_xb, d_attn_ctx))
        down_proj = (down_total + jnp.concatenate([out_xa, out_xb], axis=0)).astype(jnp.bfloat16)
        layer_out = (resid_float + down_proj.astype(jnp.float32)).astype(jnp.bfloat16).reshape(hidden.shape)
        d_qkv, grad_qgain, grad_kgain = attention_backward(d_attn_ctx, qkv, tables, heads, kv_heads, seq_len)
        qkv_part = matmul_tn(normed, d_qkv) * inv_tokens
        d_resid_late, _ = lax.optimization_barrier((d_resid_bf, qkv_part))
        blk = [attn_ctx[:, j * rows:(j + 1) * rows] for j in range(8)]
        keep, send = pick(c_bit, jnp.concatenate(blk[0::2], axis=1), jnp.concatenate(blk[1::2], axis=1))
        part = matmul_tn(send, d_resid_late)
        part = swap(part, CORE)
        part = part + matmul_tn(keep, d_resid_late)
        keep, send = pick(y_bit, part[:2 * rows], part[2 * rows:])
        part = keep + swap(send, YDIR)
        keep, send = pick(x_bit, part[:rows], part[rows:])
        grad_wo = (keep + swap(send, XDIR)) * inv_tokens
        grad_qkv = lax.psum_scatter(qkv_part, axis_name, scatter_dimension=0, tiled=True)
        grad_wq, grad_wk, grad_wv = jnp.split(grad_qkv, (w_q.shape[1], w_q.shape[1] + w_k.shape[1]), axis=1)
        d_normed = matmul_nt(d_qkv, full_qkv)
        grad_norm1 = jnp.sum(d_normed * x_unit, axis=0)
        d_hidden = (d_resid + norm_backward(d_normed * gain1, x_unit, x_scale)).astype(jnp.bfloat16).reshape(hidden.shape)

        small = jnp.concatenate([grad_norm1, grad_norm2, grad_qgain, grad_kgain]) * inv_tokens
        for mask in (CORE, XDIR, YDIR):
            small = small + swap(small, mask)
        own1 = lax.dynamic_slice_in_dim(small, me * rows, rows)
        own2 = lax.dynamic_slice_in_dim(small, width + me * rows, rows)
        gq = small[2 * width:2 * width + head_dim]
        gk = small[2 * width + head_dim:]
        return (layer_out, d_hidden, own1, own2, gq, gk, grad_wq, grad_wk, grad_wv, grad_wo, grad_gate, grad_up, grad_down)

    return jax.shard_map(device_step, mesh=mesh, in_specs=in_specs, out_specs=out_specs, check_vma=False)
```
